32 devices in a mesh: gx: 4 (over x, core), gy: 8 (over z, y).
Axes of the slice: x: 2, y: 2, z: 4, core: 2. Of those that a mesh axis runs over, the one named last changes fastest.
Arguments:
- slot_tiles: int32 [32, 32], P(('gx', 'gy')), may hold values from -1 to 63, as said below
- owner_map: int32 [32], replicated, may hold values from 0 to 31, each once
- slot_depth: int32 [32, 32, 16, 128], P(('gx', 'gy')), may hold values from 0 to 1073741823
- slot_color: bfloat16 [32, 32, 16, 3, 128], P(('gx', 'gy')), may hold values from 0 to 1
Outputs:
- region_depth: int32 [32, 2, 16, 128], P(('gx', 'gy'))
- region_color: bfloat16 [32, 2, 16, 3, 128], P(('gx', 'gy'))
- thumbnail: float32 [32, 3, 64], replicated
The draws below stay inside these ranges and needn't reach their ends.
Inputs may be any that keep to these rules, and one draw needn't show every extreme that they name: `slot_tiles`: each rank's used slots name the tiles of one rectangle of at least 4 tile rows of the 8 x 8 tile grid, each once, in row-major order, followed by -1 in the unused slots; all ranks' rectangles contain a common region. `owner_map`: each rank owns exactly one region.
All inputs are finite; a program needn't handle non-finite values.
Results may differ from the reference program's by a relative error of at most 0.001.
Values may be sent and summed in bfloat16 or wider, within the bound.
A program may use at most 64 MiB of HBM per device.

```python
import jax
import jax.numpy as jnp
from jax import lax

TILE = 128
BAND = 16
TROWS = 8
TCOLS = 8
TILES = 64
SLOTS = 32
REGIONS = 32
THUMB = 64
DEVICES = 32


def box_tiles(key):
    keys = jax.random.split(jax.random.fold_in(key, 11), 9)
    focus_pair = jax.random.randint(keys[0], (), 0, TROWS // 2)
    focus_col = jax.random.randint(keys[1], (), 0, TCOLS)
    lowest = max(3, TROWS // 2)
    box_height = lowest + jax.random.randint(keys[2], (DEVICES,), 0, 1 << 20) % (TROWS - lowest + 1)
    widest = jnp.minimum(SLOTS // box_height, TCOLS)
    narrowing = jax.random.randint(keys[8], (DEVICES,), 0, 2)
    box_width = jnp.maximum(1, widest - narrowing)
    row_low = jnp.maximum(0, 2 * focus_pair + 2 - box_height)
    row_high = jnp.minimum(2 * focus_pair, TROWS - box_height)
    row_span = row_high - row_low + 1
    first_draw = jax.random.randint(keys[4], (DEVICES,), 0, 1 << 20) % row_span
    second_draw = jax.random.randint(keys[5], (DEVICES,), 0, 1 << 20) % row_span
    top_row = row_low + (first_draw + second_draw) // 2
    col_low = jnp.maximum(0, focus_col - box_width + 1)
    col_high = jnp.minimum(focus_col, TCOLS - box_width)
    col_span = col_high - col_low + 1
    third_draw = jax.random.randint(keys[6], (DEVICES,), 0, 1 << 20) % col_span
    fourth_draw = jax.random.randint(keys[7], (DEVICES,), 0, 1 << 20) % col_span
    left_col = col_low + (third_draw + fourth_draw) // 2
    slot_index = jnp.arange(SLOTS, dtype=jnp.int32)[None, :]
    inner_row = slot_index // box_width[:, None]
    inner_col = slot_index % box_width[:, None]
    is_live = slot_index < (box_height * box_width)[:, None]
    tile_ids = (top_row[:, None] + inner_row) * TCOLS + left_col[:, None] + inner_col
    return jnp.where(is_live, tile_ids, -1).astype(jnp.int32)


def draw_slot_tiles(key, part):
    return box_tiles(key)


def draw_slot_depth(key, part):
    tile_ids = box_tiles(key)
    keys = jax.random.split(jax.random.fold_in(key, 23), 3)
    surface = jax.random.randint(keys[0], (TILES, BAND, TILE), 0, 1073741823).astype(jnp.int32)
    safe_tile = jnp.where(tile_ids >= 0, tile_ids, 0).astype(jnp.int32)
    front = surface[safe_tile]
    coin = jax.random.randint(keys[1], (DEVICES, SLOTS, BAND, TILE), 0, 8)
    room = (1073741823 - front).astype(jnp.int32)
    raw_extra = jax.random.randint(keys[2], (DEVICES, SLOTS, BAND, TILE), 0, 1 << 30).astype(jnp.int32)
    extra = 1 + raw_extra % room
    return (front + jnp.where(coin == 0, 0, extra)).astype(jnp.int32)


def block_levels(own_key, extent, shards, least, top_value):
    factor_of, own = 1.0, jax.random.fold_in(own_key, 6)
    for position, parts in shards:
        steps = jnp.exp(jax.random.uniform(jax.random.fold_in(own, position), (parts,), jnp.float32, least / len(shards), top_value / len(shards)))
        factor_of = factor_of * jnp.repeat(steps, extent[position] // parts).reshape([-1 if axis == position else 1 for axis in range(len(extent))])
    return factor_of


def setup_inputs(seed: int = 0) -> dict:
    seeds = jax.random.split(jax.random.key(seed), 5)
    return {
        "slot_tiles": draw_slot_tiles(jax.random.fold_in(seeds[4], 71), 0),
        "owner_map": jax.random.permutation(seeds[1], REGIONS).astype(jnp.int32),
        "slot_depth": draw_slot_depth(jax.random.fold_in(seeds[4], 71), 0),
        "slot_color": jnp.clip(1.0 * jax.random.uniform(seeds[3], (DEVICES, SLOTS, BAND, 3, TILE), jnp.float32) ** block_levels(seeds[3], (DEVICES, SLOTS, BAND, 3, TILE), ((0, 32),), -0.2, 0.2), 0.0, 1.0).astype(jnp.bfloat16),
    }


far_depth = 1073741824


def reference(slot_tiles, owner_map, slot_depth, slot_color):
    tile_count = TROWS * TCOLS

    def place_rank(frame_state, rank_data):
        frame_depth, frame_color = frame_state
        rank_tiles, rank_depth, rank_color = rank_data
        gather_index = jnp.where(rank_tiles >= 0, rank_tiles, tile_count).astype(jnp.int32)
        current = frame_depth[gather_index]
        nearer = rank_depth < current
        new_depth = jnp.where(nearer, rank_depth, current)
        new_color = jnp.where(nearer[:, :, None, :], rank_color, frame_color[gather_index])
        return (frame_depth.at[gather_index].set(new_depth), frame_color.at[gather_index].set(new_color)), None

    start_depth = jnp.full((tile_count + 1, BAND, TILE), far_depth, jnp.int32)
    start_color = jnp.zeros((tile_count + 1, BAND, 3, TILE), jnp.bfloat16)
    final_state, unused = lax.scan(place_rank, (start_depth, start_color), (slot_tiles, slot_depth, slot_color))
    frame_depth = final_state[0][:tile_count]
    frame_color = final_state[1][:tile_count]
    by_region_depth = jnp.transpose(frame_depth.reshape(TROWS // 2, 2, TCOLS, BAND, TILE), (0, 2, 1, 3, 4)).reshape(REGIONS, 2, BAND, TILE)
    by_region_color = jnp.transpose(frame_color.reshape(TROWS // 2, 2, TCOLS, BAND, 3, TILE), (0, 2, 1, 3, 4, 5)).reshape(REGIONS, 2, BAND, 3, TILE)
    inverse = jnp.zeros((REGIONS,), jnp.int32).at[owner_map].set(jnp.arange(REGIONS, dtype=jnp.int32))
    region_depth = by_region_depth[inverse]
    region_color = by_region_color[inverse]
    block_means = by_region_color.astype(jnp.float32).reshape(REGIONS, 2, BAND // 8, 8, 3, TILE // 8, 8).mean(axis=(3, 6))
    thumbnail = jnp.transpose(block_means, (0, 3, 1, 2, 4)).reshape(REGIONS, 3, THUMB)
    return region_depth, region_color, thumbnail
```

```python
import functools

import jax
import jax.numpy as jnp
from jax import lax
from jax.experimental import pallas as pl
from jax.experimental.pallas import tpu as pltpu
from jax.sharding import PartitionSpec as P

FAR = 1073741824
HALF = 536870912
LOWEST = -2147483648
MESH = pl.DeviceIdType.MESH


def div_const(value, by):
    if by & (by - 1) == 0:
        return value >> (by.bit_length() - 1)
    return value // by


def merge(first, second):
    key_a, colors_a = first
    key_b, colors_b = second
    nearer = key_b < key_a
    key = jnp.where(nearer, key_b, key_a)
    return key, [jnp.where(nearer, b, a) for a, b in zip(colors_a, colors_b)]


def kernel(
    dims, inv_ref, own_ref, slots_ref, depth_ref, color_ref,
    out_d, out_c, out_t,
    cs_d, cs_c, cr_d, cr_c, ys_d, ys_c, yr_d, yr_c, zs_d, zs_c, zr_d, zr_c, xs_d, xs_c, xr_d, xr_c,
    gath,
    c_ss, c_rs, y_ss, y_rs, z_ss, z_rs, x_ss, x_rs, g1_ss, g1_rs, g2_ss, g2_rs,
):
    GX, GY, X, Y, Z = dims
    regions = GX * GY
    gx = lax.axis_index("gx")
    gy = lax.axis_index("gy")
    core = lax.rem(gx, 2)
    x = lax.div(gx, 2)
    y = lax.rem(gy, Y)
    z = lax.div(gy, Y)
    tile_cols = GY

    barrier = pltpu.get_barrier_semaphore()
    for j in range(1, GX):
        pl.semaphore_signal(barrier, inc=1, device_id=(lax.rem(gx + j, GX), gy), device_id_type=MESH)
    for j in range(1, GY):
        pl.semaphore_signal(barrier, inc=1, device_id=(gx, lax.rem(gy + j, GY)), device_id_type=MESH)

    first = slots_ref[0, 0]
    last = first
    for s in range(1, slots_ref.shape[1]):
        last = jnp.maximum(last, slots_ref[0, s])
    top = div_const(first, tile_cols)
    left = first - top * tile_cols
    bottom = div_const(last, tile_cols)
    right = last - bottom * tile_cols
    width = right - left + 1

    def own_tile(owner_core, owner_x, owner_y, owner_z, half):
        rank = (owner_x * 2 + owner_core) * GY + owner_z * Y + owner_y
        region = inv_ref[rank]
        pair = div_const(region, tile_cols)
        col = region - pair * tile_cols
        row = pair * 2 + half
        live = (row >= top) & (row <= bottom) & (col >= left) & (col <= right)
        slot = jnp.where(live, (row - top) * width + (col - left), 0)
        floor = jnp.where(live, LOWEST, 2 * HALF)
        key = jnp.maximum((depth_ref[slot] - HALF) * 2, floor) + core
        return key, [color_ref[slot, c] for c in range(3)]

    def load(ref_d, ref_c, index):
        return ref_d[index], [ref_c[index + (c,)] for c in range(3)]

    def store(ref_d, ref_c, index, value):
        ref_d[index] = value[0]
        for c in range(3):
            ref_c[index + (c,)] = value[1][c]

    pending = []

    def remote(src, dst, ss, rs, device):
        return pltpu.make_async_remote_copy(
            src_ref=src, dst_ref=dst, send_sem=ss, recv_sem=rs, device_id=device, device_id_type=MESH
        )

    def send(pairs, sems, device):
        for k, (src, dst) in enumerate(pairs):
            copy = remote(src, dst, sems[0].at[sems[1] + (k,)], sems[2].at[sems[3] + (k,)], device)
            copy.start()
            pending.append(copy)

    def arrived(refs, rs, index, device):
        for k, ref in enumerate(refs):
            remote(ref, ref, c_ss.at[0, k], rs.at[index + (k,)], device).wait_recv()

    other_core = 1 - core
    core_partner = (x * 2 + other_core, gy)
    me = (gx, gy)
    chunk_x = [lax.rem(x + 1 + j, X) for j in range(X)]

    for j in range(X):

        def pack(i, carry, j=j):
            yy = lax.div(i, Z)
            zz = lax.rem(i, Z)
            for h in range(2):
                store(cs_d, cs_c, (j, yy, zz, h), own_tile(other_core, chunk_x[j], yy, zz, h))
            return carry

        lax.fori_loop(0, Y * Z, pack, 0)
        if j == 0:
            pl.semaphore_wait(barrier, GX + GY - 2)
        send([(cs_d.at[j], cr_d.at[j]), (cs_c.at[j], cr_c.at[j])], (c_ss, (j,), c_rs, (j,)), core_partner)

    lane_k = lax.broadcasted_iota(jnp.int32, (128, 128), 0) // 8
    lane_l = lax.broadcasted_iota(jnp.int32, (128, 128), 1)
    groups = []
    for h in range(2):
        hit = (lane_l == lane_k + 32 * h) | (lane_l == lane_k + 32 * h + 80)
        groups.append(jnp.where(hit, 1.0 / 64.0, 0.0).astype(jnp.bfloat16))

    for j in range(X):
        arrived([cr_d.at[j], cr_c.at[j]], c_rs, (j,), me)
        for i in range(Y):
            yy = lax.rem(y + 1 + i, Y)
            mine = i == Y - 1

            def step(zz, carry, j=j, yy=yy, mine=mine):
                for h in range(2):
                    value = merge(
                        own_tile(core, chunk_x[j], yy, zz, h), load(cr_d, cr_c, (j, yy, zz, h))
                    )
                    if mine:
                        store(yr_d, yr_c, (j, y, zz, h), value)
                    else:
                        store(ys_d, ys_c, (j, yy, zz, h), value)
                return carry

            lax.fori_loop(0, Z, step, 0)
            if not mine:
                send(
                    [(ys_d.at[j, yy], yr_d.at[j, y]), (ys_c.at[j, yy], yr_c.at[j, y])],
                    (y_ss, (j, i), y_rs, (j, y)),
                    (gx, z * Y + yy),
                )

    for j in range(X):
        for i in range(Y - 1):
            yy = lax.rem(y + 1 + i, Y)
            arrived([yr_d.at[j, yy], yr_c.at[j, yy]], y_rs, (j, yy), me)
        for i in range(Z):
            zz = lax.rem(z + 1 + i, Z)
            mine = i == Z - 1
            for h in range(2):
                value = load(yr_d, yr_c, (j, 0, zz, h))
                for k in range(1, Y):
                    value = merge(value, load(yr_d, yr_c, (j, k, zz, h)))
                if mine:
                    store(zr_d, zr_c, (j, z, h), value)
                else:
                    store(zs_d, zs_c, (j, zz, h), value)
            if not mine:
                send(
                    [(zs_d.at[j, zz], zr_d.at[j, z]), (zs_c.at[j, zz], zr_c.at[j, z])],
                    (z_ss, (j, i), z_rs, (j, z)),
                    (gx, zz * Y + y),
                )

    for j in range(X):
        for i in range(Z - 1):
            zz = lax.rem(z + 1 + i, Z)
            arrived([zr_d.at[j, zz], zr_c.at[j, zz]], z_rs, (j, zz), me)
        mine = j == X - 1
        for h in range(2):
            value = load(zr_d, zr_c, (j, 0, h))
            for k in range(1, Z):
                value = merge(value, load(zr_d, zr_c, (j, k, h)))
            value = (value[0] >> 1, value[1])
            if mine:
                store(xr_d, xr_c, (x, h), value)
            else:
                store(xs_d, xs_c, (j, h), value)
        if not mine:
            send(
                [(xs_d.at[j], xr_d.at[x]), (xs_c.at[j], xr_c.at[x])],
                (x_ss, (j,), x_rs, (x,)),
                (chunk_x[j] * 2 + core, gy),
            )

    for j in range(X - 1):
        xx = chunk_x[j]
        arrived([xr_d.at[xx], xr_c.at[xx]], x_rs, (xx,), me)

    sums = [None] * 3
    row = lax.broadcasted_iota(jnp.int32, (16, 128), 0)
    lane = lax.broadcasted_iota(jnp.int32, (16, 128), 1)
    keep = (row < 8) == (lane < 64)
    for h in range(2):
        value = load(xr_d, xr_c, (0, h))
        for k in range(1, X):
            value = merge(value, load(xr_d, xr_c, (k, h)))
        depth = value[0] + HALF
        out_d[h] = depth
        for c in range(3):
            color = jnp.where(depth == FAR, jnp.zeros((), jnp.bfloat16), value[1][c])
            out_c[h, c] = color
            part = jnp.dot(color, groups[h], preferred_element_type=jnp.float32)
            part = jnp.where(keep, part, 0.0)
            sums[c] = part if sums[c] is None else sums[c] + part
    rows = []
    for c in range(3):
        total = jnp.sum(sums[c], axis=0, keepdims=True)
        rows.append(total + pltpu.roll(total, 64, 1))
    lane_row = lax.broadcasted_iota(jnp.int32, (1, 128), 1)
    gath[gy, gx, 0:1, :] = jnp.where(lane_row < 64, rows[0], rows[1])
    gath[gy, gx, 1:2, :] = rows[2]

    for j in range(1, GX):
        send([(gath.at[gy, gx], gath.at[gy, gx])], (g1_ss, (j,), g1_rs, (gx,)), (lax.rem(gx + j, GX), gy))
    for j in range(1, GX):
        xx = lax.rem(gx + j, GX)
        arrived([gath.at[gy, xx]], g1_rs, (xx,), me)
    for j in range(1, GY):
        send([(gath.at[gy], gath.at[gy])], (g2_ss, (j,), g2_rs, (gy,)), (gx, lax.rem(gy + j, GY)))
    for j in range(1, GY):
        yy = lax.rem(gy + j, GY)
        arrived([gath.at[yy]], g2_rs, (yy,), me)

    def place(r, carry):
        owner = own_ref[r]
        owner_x = div_const(owner, GY)
        out_t[r] = gath[owner - owner_x * GY, owner_x]
        return carry

    lax.fori_loop(0, regions, place, 0)
    for copy in pending:
        copy.wait_send()


def shards(slot_tiles, owner_map, slot_depth, slot_color):
    GX = lax.axis_size("gx")
    GY = lax.axis_size("gy")
    X, Z = GX // 2, 4
    Y = GY // Z
    regions = GX * GY
    band, width = slot_depth.shape[2:]
    ids = jnp.arange(regions, dtype=jnp.int32)
    inverse = jnp.sum(jnp.where(owner_map[None, :] == ids[:, None], ids[None, :], 0), axis=1)
    depth = slot_depth[0]
    color = jnp.transpose(slot_color[0], (0, 2, 1, 3))

    def pair(*lead):
        return [
            pltpu.VMEM(lead + (2, band, width), jnp.int32),
            pltpu.VMEM(lead + (2, 3, band, width), jnp.bfloat16),
        ]

    dma = lambda *shape: pltpu.SemaphoreType.DMA(shape)
    vmem = pl.BlockSpec(memory_space=pltpu.VMEM)
    smem = pl.BlockSpec(memory_space=pltpu.SMEM)
    out_d, out_c, out_t = pl.pallas_call(
        functools.partial(kernel, (GX, GY, X, Y, Z)),
        out_shape=(
            jax.ShapeDtypeStruct((2, band, width), jnp.int32),
            jax.ShapeDtypeStruct((2, 3, band, width), jnp.bfloat16),
            jax.ShapeDtypeStruct((regions, 2, width), jnp.float32),
        ),
        in_specs=[smem, smem, smem, vmem, vmem],
        out_specs=(vmem, vmem, vmem),
        scratch_shapes=[
            *pair(X, Y, Z), *pair(X, Y, Z),
            *pair(X, Y, Z), *pair(X, Y, Z),
            *pair(X, Z), *pair(X, Z),
            *pair(X), *pair(X),
            pltpu.VMEM((GY, GX, 2, width), jnp.float32),
            dma(X, 2), dma(X, 2),
            dma(X, Y, 2), dma(X, Y, 2),
            dma(X, Z, 2), dma(X, Z, 2),
            dma(X, 2), dma(X, 2),
            dma(GX, 1), dma(GX, 1),
            dma(GY, 1), dma(GY, 1),
        ],
        compiler_params=pltpu.CompilerParams(collective_id=0, has_side_effects=True),
    )(inverse, owner_map, slot_tiles, depth, color)
    thumbnail = out_t.reshape(regions, 2 * width)[:, : 3 * width // 2].reshape(regions, 3, width // 2)
    return (out_d[None], jnp.transpose(out_c, (0, 2, 1, 3))[None], thumbnail)


def solution(mesh):
    placed = (
        P(("gx", "gy"), None),
        P(),
        P(("gx", "gy"), None, None, None),
        P(("gx", "gy"), None, None, None, None),
    )
    return jax.shard_map(
        shards,
        mesh=mesh,
        in_specs=placed,
        out_specs=(P(("gx", "gy"), None, None, None), P(("gx", "gy"), None, None, None, None), P()),
        check_vma=False,
    )
```

```python
import functools

import jax
import jax.numpy as jnp
from jax import lax
from jax.experimental import pallas as pl
from jax.experimental.pallas import tpu as pltpu
from jax.sharding import PartitionSpec as P

FAR = 1073741824
HALF = 536870912
LOWEST = -2147483648
MESH = pl.DeviceIdType.MESH


def div_const(value, by):
    if by & (by - 1) == 0:
        return value >> (by.bit_length() - 1)
    return value // by


def merge(first, second):
    key_a, colors_a = first
    key_b, colors_b = second
    nearer = key_b < key_a
    key = jnp.where(nearer, key_b, key_a)
    return key, [jnp.where(nearer, b, a) for a, b in zip(colors_a, colors_b)]


def kernel(
    dims, inv_ref, own_ref, slots_ref, depth_ref, color_ref,
    out_d, out_c, out_t,
    cs_d, cs_c, cr_d, cr_c, ys_d, ys_c, yr_d, yr_c, zs_d, zs_c, zr_d, zr_c, xs_d, xs_c, xr_d, xr_c,
    gath,
    c_ss, c_rs, y_ss, y_rs, z_ss, z_rs, x_ss, x_rs, g1_ss, g1_rs, g2_ss, g2_rs,
):
    GX, GY, X, Y, Z = dims
    regions = GX * GY
    gx = lax.axis_index("gx")
    gy = lax.axis_index("gy")
    core = lax.rem(gx, 2)
    x = lax.div(gx, 2)
    y = lax.rem(gy, Y)
    z = lax.div(gy, Y)
    tile_cols = GY

    barrier = pltpu.get_barrier_semaphore()
    for j in range(1, GX):
        pl.semaphore_signal(barrier, inc=1, device_id=(lax.rem(gx + j, GX), gy), device_id_type=MESH)
    for j in range(1, GY):
        pl.semaphore_signal(barrier, inc=1, device_id=(gx, lax.rem(gy + j, GY)), device_id_type=MESH)

    first = slots_ref[0, 0]
    last = first
    for s in range(1, slots_ref.shape[1]):
        last = jnp.maximum(last, slots_ref[0, s])
    top = div_const(first, tile_cols)
    left = first - top * tile_cols
    bottom = div_const(last, tile_cols)
    right = last - bottom * tile_cols
    width = right - left + 1

    def own_tile(owner_core, owner_x, owner_y, owner_z, half):
        rank = (owner_x * 2 + owner_core) * GY + owner_z * Y + owner_y
        region = inv_ref[rank]
        pair = div_const(region, tile_cols)
        col = region - pair * tile_cols
        row = pair * 2 + half
        live = (row >= top) & (row <= bottom) & (col >= left) & (col <= right)
        slot = jnp.where(live, (row - top) * width + (col - left), 0)
        floor = jnp.where(live, LOWEST, 2 * HALF)
        key = jnp.maximum((depth_ref[slot] - HALF) * 2, floor) + core
        return key, [color_ref[slot, c] for c in range(3)]

    def load(ref_d, ref_c, index):
        return ref_d[index], [ref_c[index + (c,)] for c in range(3)]

    def store(ref_d, ref_c, index, value):
        ref_d[index] = value[0]
        for c in range(3):
            ref_c[index + (c,)] = value[1][c]

    pending = []

    def remote(src, dst, ss, rs, device):
        return pltpu.make_async_remote_copy(
            src_ref=src, dst_ref=dst, send_sem=ss, recv_sem=rs, device_id=device, device_id_type=MESH
        )

    def send(pairs, sems, device):
        for k, (src, dst) in enumerate(pairs):
            copy = remote(src, dst, sems[0].at[sems[1] + (k,)], sems[2].at[sems[3] + (k,)], device)
            copy.start()
            pending.append(copy)

    def arrived(refs, rs, index, device):
        for k, ref in enumerate(refs):
            remote(ref, ref, c_ss.at[0, k], rs.at[index + (k,)], device).wait_recv()

    other_core = 1 - core
    core_partner = (x * 2 + other_core, gy)
    me = (gx, gy)
    chunk_x = [lax.rem(x + 1 + j, X) for j in range(X)]

    for j in range(X):

        def pack(i, carry, j=j):
            yy = lax.div(i, Z)
            zz = lax.rem(i, Z)
            for h in range(2):
                store(cs_d, cs_c, (j, yy, zz, h), own_tile(other_core, chunk_x[j], yy, zz, h))
            return carry

        lax.fori_loop(0, Y * Z, pack, 0)
        if j == 0:
            pl.semaphore_wait(barrier, GX + GY - 2)
        send([(cs_d.at[j], cr_d.at[j]), (cs_c.at[j], cr_c.at[j])], (c_ss, (j,), c_rs, (j,)), core_partner)

    lane_k = lax.broadcasted_iota(jnp.int32, (128, 128), 0) // 8
    lane_l = lax.broadcasted_iota(jnp.int32, (128, 128), 1)
    groups = []
    for h in range(2):
        hit = (lane_l == lane_k + 32 * h) | (lane_l == lane_k + 32 * h + 80)
        groups.append(jnp.where(hit, 1.0 / 64.0, 0.0).astype(jnp.bfloat16))

    for j in range(X):
        arrived([cr_d.at[j], cr_c.at[j]], c_rs, (j,), me)
        for i in range(Y):
            yy = lax.rem(y + 1 + i, Y)
            mine = i == Y - 1

            def step(zz, carry, j=j, yy=yy, mine=mine):
                for h in range(2):
                    value = merge(
                        own_tile(core, chunk_x[j], yy, zz, h), load(cr_d, cr_c, (j, yy, zz, h))
                    )
                    if mine:
                        store(yr_d, yr_c, (j, y, zz, h), value)
                    else:
                        store(ys_d, ys_c, (j, yy, zz, h), value)
                return carry

            lax.fori_loop(0, Z, step, 0)
            if not mine:
                send(
                    [(ys_d.at[j, yy], yr_d.at[j, y]), (ys_c.at[j, yy], yr_c.at[j, y])],
                    (y_ss, (j, i), y_rs, (j, y)),
                    (gx, z * Y + yy),
                )

    for j in range(X):
        for i in range(Y - 1):
            yy = lax.rem(y + 1 + i, Y)
            arrived([yr_d.at[j, yy], yr_c.at[j, yy]], y_rs, (j, yy), me)
        for i in range(Z):
            zz = lax.rem(z + 1 + i, Z)
            mine = i == Z - 1
            for h in range(2):
                value = load(yr_d, yr_c, (j, 0, zz, h))
                for k in range(1, Y):
                    value = merge(value, load(yr_d, yr_c, (j, k, zz, h)))
                if mine:
                    store(zr_d, zr_c, (j, z, h), value)
                else:
                    store(zs_d, zs_c, (j, zz, h), value)
            if not mine:
                send(
                    [(zs_d.at[j, zz], zr_d.at[j, z]), (zs_c.at[j, zz], zr_c.at[j, z])],
                    (z_ss, (j, i), z_rs, (j, z)),
                    (gx, zz * Y + y),
                )

    for j in range(X):
        for i in range(Z - 1):
            zz = lax.rem(z + 1 + i, Z)
            arrived([zr_d.at[j, zz], zr_c.at[j, zz]], z_rs, (j, zz), me)
        mine = j == X - 1
        for h in range(2):
            value = load(zr_d, zr_c, (j, 0, h))
            for k in range(1, Z):
                value = merge(value, load(zr_d, zr_c, (j, k, h)))
            value = (value[0] >> 1, value[1])
            if mine:
                store(xr_d, xr_c, (x, h), value)
            else:
                store(xs_d, xs_c, (j, h), value)
        if not mine:
            send(
                [(xs_d.at[j], xr_d.at[x]), (xs_c.at[j], xr_c.at[x])],
                (x_ss, (j,), x_rs, (x,)),
                (chunk_x[j] * 2 + core, gy),
            )

    for j in range(X - 1):
        xx = chunk_x[j]
        arrived([xr_d.at[xx], xr_c.at[xx]], x_rs, (xx,), me)

    sums = [None] * 3
    row = lax.broadcasted_iota(jnp.int32, (16, 128), 0)
    lane = lax.broadcasted_iota(jnp.int32, (16, 128), 1)
    keep = (row < 8) == (lane < 64)
    for h in range(2):
        value = load(xr_d, xr_c, (0, h))
        for k in range(1, X):
            value = merge(value, load(xr_d, xr_c, (k, h)))
        depth = value[0] + HALF
        out_d[h] = depth
        for c in range(3):
            color = jnp.where(depth == FAR, jnp.zeros((), jnp.bfloat16), value[1][c])
            out_c[h, c] = color
            part = jnp.dot(color, groups[h], preferred_element_type=jnp.float32)
            part = jnp.where(keep, part, 0.0)
            sums[c] = part if sums[c] is None else sums[c] + part
    rows = []
    for c in range(3):
        total = jnp.sum(sums[c], axis=0, keepdims=True)
        rows.append(total + pltpu.roll(total, 64, 1))
    lane_row = lax.broadcasted_iota(jnp.int32, (1, 128), 1)
    gath[gy, gx, 0:1, :] = jnp.where(lane_row < 64, rows[0], rows[1])
    gath[gy, gx, 1:2, :] = rows[2]

    for j in range(1, GX):
        send([(gath.at[gy, gx], gath.at[gy, gx])], (g1_ss, (j,), g1_rs, (gx,)), (lax.rem(gx + j, GX), gy))
    for j in range(1, GX):
        xx = lax.rem(gx + j, GX)
        arrived([gath.at[gy, xx]], g1_rs, (xx,), me)
    for j in range(1, GY):
        send([(gath.at[gy], gath.at[gy])], (g2_ss, (j,), g2_rs, (gy,)), (gx, lax.rem(gy + j, GY)))
    for j in range(1, GY):
        yy = lax.rem(gy + j, GY)
        arrived([gath.at[yy]], g2_rs, (yy,), me)

    def place(r, carry):
        owner = own_ref[r]
        owner_x = div_const(owner, GY)
        out_t[r] = gath[owner - owner_x * GY, owner_x]
        return carry

    lax.fori_loop(0, regions, place, 0)
    for copy in pending:
        copy.wait_send()


def finish(in_d, in_c, in_t, out_d, out_c, out_t):
    out_d[...] = in_d[...]
    out_c[...] = in_c[...]
    side = out_t.shape[2]
    upper = in_t[:, 0, :]
    out_t[0] = upper[:, :side]
    out_t[1] = upper[:, side:]
    out_t[2] = in_t[:, 1, :][:, :side]


def shards(slot_tiles, owner_map, slot_depth, slot_color):
    GX = lax.axis_size("gx")
    GY = lax.axis_size("gy")
    X, Z = GX // 2, 4
    Y = GY // Z
    regions = GX * GY
    band, width = slot_depth.shape[2:]
    ids = jnp.arange(regions, dtype=jnp.int32)
    inverse = jnp.sum(jnp.where(owner_map[None, :] == ids[:, None], ids[None, :], 0), axis=1)
    depth = slot_depth[0]
    color = jnp.transpose(slot_color[0], (0, 2, 1, 3))

    def pair(*lead):
        return [
            pltpu.VMEM(lead + (2, band, width), jnp.int32),
            pltpu.VMEM(lead + (2, 3, band, width), jnp.bfloat16),
        ]

    dma = lambda *shape: pltpu.SemaphoreType.DMA(shape)
    vmem = pl.BlockSpec(memory_space=pltpu.VMEM)
    smem = pl.BlockSpec(memory_space=pltpu.SMEM)
    out_d, out_c, out_t = pl.pallas_call(
        functools.partial(kernel, (GX, GY, X, Y, Z)),
        out_shape=(
            jax.ShapeDtypeStruct((2, band, width), jnp.int32),
            jax.ShapeDtypeStruct((2, 3, band, width), jnp.bfloat16),
            jax.ShapeDtypeStruct((regions, 2, width), jnp.float32),
        ),
        in_specs=[smem, smem, smem, vmem, vmem],
        out_specs=(vmem, vmem, vmem),
        scratch_shapes=[
            *pair(X, Y, Z), *pair(X, Y, Z),
            *pair(X, Y, Z), *pair(X, Y, Z),
            *pair(X, Z), *pair(X, Z),
            *pair(X), *pair(X),
            pltpu.VMEM((GY, GX, 2, width), jnp.float32),
            dma(X, 2), dma(X, 2),
            dma(X, Y, 2), dma(X, Y, 2),
            dma(X, Z, 2), dma(X, Z, 2),
            dma(X, 2), dma(X, 2),
            dma(GX, 1), dma(GX, 1),
            dma(GY, 1), dma(GY, 1),
        ],
        compiler_params=pltpu.CompilerParams(collective_id=0, has_side_effects=True),
    )(inverse, owner_map, slot_tiles, depth, color)
    out_d, out_c, out_t = pl.pallas_call(
        finish,
        out_shape=(
            jax.ShapeDtypeStruct((2, band, width), jnp.int32),
            jax.ShapeDtypeStruct((2, 3, band, width), jnp.bfloat16),
            jax.ShapeDtypeStruct((3, regions, width // 2), jnp.float32),
        ),
        in_specs=[vmem, vmem, vmem],
        out_specs=(vmem, vmem, vmem),
    )(out_d, out_c, out_t)
    thumbnail = jnp.transpose(out_t, (1, 0, 2))
    return (out_d[None], jnp.transpose(out_c, (0, 2, 1, 3))[None], thumbnail)


def solution(mesh):
    placed = (
        P(("gx", "gy"), None),
        P(),
        P(("gx", "gy"), None, None, None),
        P(("gx", "gy"), None, None, None, None),
    )
    return jax.shard_map(
        shards,
        mesh=mesh,
        in_specs=placed,
        out_specs=(P(("gx", "gy"), None, None, None), P(("gx", "gy"), None, None, None, None), P()),
        check_vma=False,
    )
```
